32 devices in a mesh: dp: 8 (over z, x), mp: 4 (over y, core).
Axes of the slice: x: 2, y: 2, z: 4, core: 2. Of those that a mesh axis runs over, the one named last changes fastest.
Arguments:
- tokens: bfloat16 [1024, 4096], P('dp'), may hold values from -6 to 6
- cotangent: bfloat16 [1024, 4096], P('dp', 'mp'), may hold values from -6 to 6
- sketch: float32 [4096, 128], P('dp'), may hold values from -12 to 12
Outputs:
- precond: bfloat16 [4096, 4096], P('dp', 'mp')
- new_sketch: float32 [4096, 128], P('dp')
The draws below stay inside these ranges and needn't reach their ends.
All inputs are finite; a program needn't handle non-finite values.
Results may differ from the reference program's by a relative error of at most 0.001.
Values sent between devices are 32-bit elements; how exact they have to be, the bound alone decides.
A program may use at most 64 MiB of HBM per device.

```python
import math
import jax
import jax.numpy as jnp
from jax import lax

D = 4096
COLS = 4096
RANK = 128
ITERS = 1
TOKENS = 1024


def strengthened(entries, stream_key, source, target, blocks, factor):
    owner, partner = [(jnp.arange(entries.shape[position]) // (entries.shape[position] // blocks)).reshape([-1 if axis == position else 1 for axis in range(entries.ndim)]) for position in (source, target)]
    chosen = jax.random.permutation(stream_key, blocks)[partner]
    strong = (owner == chosen) | (owner == (partner + blocks // 2) % blocks)
    return jnp.where(strong, factor * entries, entries)


def shard_levels(stream_key, dims, pieces, least, top_value):
    factor_of = 1.0
    for dim, shards_of in pieces:
        steps = jax.random.uniform(jax.random.fold_in(jax.random.fold_in(stream_key, 6), dim), (shards_of,), jnp.float32, least / len(pieces), top_value / len(pieces))
        factor_of = factor_of * jnp.repeat(jnp.exp(steps), dims[dim] // shards_of).reshape((-1,) + (1,) * (len(dims) - 1 - dim))
    return factor_of


def gaussian(rng, dims, deviation, most, pieces=(), kind=jnp.bfloat16):
    factor_of = shard_levels(rng, dims, pieces, -0.22, 0.18) if pieces else 1.0
    array = jax.random.normal(rng, dims, jnp.float32) * deviation * factor_of
    return jnp.minimum(jnp.maximum(array, -most), most).astype(kind)


def bell_draw_with(stream_key, dims, scale, bound, pieces, heavy, held_as=jnp.bfloat16):
    entries = scale * jax.random.normal(stream_key, dims, jnp.float32)
    if pieces:
        entries = entries * shard_levels(stream_key, dims, pieces, -0.22, 0.18)
    return jnp.clip(strengthened(entries, jax.random.fold_in(stream_key, 3), *heavy), -bound, bound).astype(held_as)


def setup_inputs(seed: int = 0) -> dict:
    streams_of = jax.random.split(jax.random.key(seed), 4)
    return {
        "tokens": bell_draw_with(streams_of[0], (TOKENS, D), 1.0, 6.0, ((0, 8),), (0, 1, 8, 2.0)),
        "cotangent": gaussian(streams_of[1], (TOKENS, COLS), 1.0, 6.0, ((0, 8), (1, 4))),
        "sketch": gaussian(streams_of[2], (D, RANK), 2.0, 12.0, ((0, 8),), jnp.float32),
    }


DECAY_RATE = 0.9
RIDGE_FRAC = 0.0001

def product(left_mat, right_mat):
    return jnp.dot(left_mat, right_mat, precision=lax.Precision.HIGHEST)

def right_solve(values, lower_tri):
    return lax.linalg.triangular_solve(lower_tri, values, left_side=False, lower=True, transpose_a=True)

def left_solve(lower_tri, values, transpose):
    return lax.linalg.triangular_solve(lower_tri, values, left_side=True, lower=True, transpose_a=transpose)

def spd_solve(matrix, target):
    lower_tri = jnp.linalg.cholesky(matrix)
    return left_solve(lower_tri, left_solve(lower_tri, target, False), True)

def reference(tokens, cotangent, sketch):
    gradient = jnp.dot(tokens.T.astype(jnp.float32), cotangent.astype(jnp.float32), preferred_element_type=jnp.float32) * (1.0 / math.sqrt(TOKENS))

    def covariance(basis_now):
        return DECAY_RATE * product(sketch, product(sketch.T, basis_now)) + product(gradient, product(gradient.T, basis_now))
    basis_now = sketch
    for iteration in range(ITERS):
        applied = covariance(basis_now)
        basis_now = right_solve(applied, jnp.linalg.cholesky(product(applied.T, applied)))
    applied = covariance(basis_now)
    rayleigh = product(basis_now.T, applied)
    rayleigh = 0.5 * (rayleigh + rayleigh.T)
    mean_level = jnp.trace(rayleigh) / RANK
    identity = jnp.eye(RANK, dtype=jnp.float32)
    new_sketch = right_solve(applied, jnp.linalg.cholesky(rayleigh + RIDGE_FRAC * mean_level * identity))
    inner_mat = mean_level * identity + product(new_sketch.T, new_sketch)
    coeffs = spd_solve(inner_mat, product(new_sketch.T, gradient))
    precond = gradient - product(new_sketch, coeffs)
    return (precond.astype(jnp.bfloat16), new_sketch)
```

```python
import functools
import math

import jax
import jax.numpy as jnp
from jax import lax
from jax.experimental import pallas as pl
from jax.experimental.pallas import tpu as pltpu
from jax.sharding import PartitionSpec as P

DECAY_RATE = 0.9
RIDGE_FRAC = 0.0001
MESH = pl.DeviceIdType.MESH
VMEM = pltpu.MemorySpace.VMEM
VMEM_BUDGET = 48 * 2**20


def product(left_mat, right_mat, dims=((1,), (0,))):
    return lax.dot_general(
        left_mat,
        right_mat,
        (dims, ((), ())),
        precision=lax.Precision.HIGHEST,
        preferred_element_type=jnp.float32,
    )


TN = ((0,), (0,))
NT = ((1,), (1,))


def remote(src, dst, send, recv, where):
    return pltpu.make_async_remote_copy(
        src_ref=src,
        dst_ref=dst,
        send_sem=send,
        recv_sem=recv,
        device_id=where,
        device_id_type=MESH,
    )


def reduce_kernel(axis, n, x_ref, o_ref, land, own, send_a, recv_a, send_b, recv_b):
    me = lax.axis_index(axis)
    chunk = own.shape[0]
    barrier = pltpu.get_barrier_semaphore()
    peers = [lax.rem(me + k, n) for k in range(1, n)]
    for peer in peers:
        pl.semaphore_signal(barrier, inc=1, device_id={axis: peer}, device_id_type=MESH)
    pl.semaphore_wait(barrier, n - 1)
    scatter = [
        remote(
            x_ref.at[pl.ds(pl.multiple_of(peer * chunk, 8), chunk)],
            land.at[k],
            send_a.at[k],
            recv_a.at[k],
            {axis: peer},
        )
        for k, peer in enumerate(peers)
    ]
    for copy in scatter:
        copy.start()
    mine = pl.ds(pl.multiple_of(me * chunk, 8), chunk)
    total = x_ref[mine]
    for k, copy in enumerate(scatter):
        copy.wait_recv()
        total = total + land[k]
    own[...] = total
    gather = [
        remote(own, o_ref.at[mine], send_b.at[k], recv_b.at[k], {axis: peer})
        for k, peer in enumerate(peers)
    ]
    for copy in gather:
        copy.start()
    o_ref[mine] = total
    for copy in scatter:
        copy.wait_send()
    for copy in gather:
        copy.wait()


def all_sum(arrays, axis, ident):
    n = lax.axis_size(axis)
    rows = sum(a.shape[0] for a in arrays)
    if rows % (8 * n) or n > 16:
        return lax.psum(tuple(arrays), axis)
    joined = arrays[0] if len(arrays) == 1 else jnp.concatenate(arrays, axis=0)
    width = joined.shape[1]
    chunk = rows // n
    summed = pl.pallas_call(
        functools.partial(reduce_kernel, axis, n),
        out_shape=jax.ShapeDtypeStruct(joined.shape, jnp.float32),
        in_specs=[pl.BlockSpec(memory_space=VMEM)],
        out_specs=pl.BlockSpec(memory_space=VMEM),
        scratch_shapes=[
            pltpu.VMEM((n - 1, chunk, width), jnp.float32),
            pltpu.VMEM((chunk, width), jnp.float32),
        ]
        + [pltpu.SemaphoreType.DMA((n - 1,))] * 4,
        compiler_params=pltpu.CompilerParams(collective_id=ident, has_side_effects=True),
        name=f"sum_{axis}_{ident}",
    )(joined)
    outs, at = [], 0
    for a in arrays:
        outs.append(summed[at : at + a.shape[0]])
        at += a.shape[0]
    return tuple(outs)


def gradient_kernel(
    nd, nm, scale, x_ref, y_ref, g_ref, xland, yland, xt, yb,
    local, xs, xr, ms, mr, zs, zr, fs, fr,
):
    d, m = lax.axis_index("dp"), lax.axis_index("mp")
    rows, block = xland.shape[1], xland.shape[2]
    share = rows // nm
    nz = nd // 2
    z, x = lax.div(d, 2), lax.rem(d, 2)
    other = 2 * z + 1 - x
    barrier = pltpu.get_barrier_semaphore()
    for k in range(1, nd):
        pl.semaphore_signal(barrier, inc=1, device_id={"dp": lax.rem(d + k, nd)}, device_id_type=MESH)
    for k in range(1, nm):
        pl.semaphore_signal(barrier, inc=1, device_id={"mp": lax.rem(m + k, nm)}, device_id_type=MESH)
    pl.semaphore_wait(barrier, nd + nm - 2)

    part = pl.ds(pl.multiple_of(m * share, 8), share)
    x_out, z_out = [], []
    for k in range(1, nd):
        peer = lax.rem(d + k, nd)
        cols = pl.ds(pl.multiple_of(peer * block, 128), block)
        x_out.append(
            remote(x_ref.at[part, cols], xland.at[d, part], xs.at[k - 1], xr.at[k - 1], {"dp": peer})
        )
    for k in range(1, nz):
        peer = 2 * lax.rem(z + k, nz) + x
        z_out.append(remote(y_ref, yland.at[d], zs.at[k - 1], zr.at[k - 1], {"dp": peer}))
    over = [remote(y_ref, yland.at[d], fs.at[0], fr.at[0], {"dp": other})]
    over[0].start()
    for copy in x_out:
        copy.start()
    for copy in z_out:
        copy.start()
    mine = pl.ds(pl.multiple_of(d * block, 128), block)
    keep_x = pltpu.make_async_copy(x_ref.at[:, mine], xland.at[d], local.at[0])
    keep_y = pltpu.make_async_copy(y_ref, yland.at[d], local.at[1])
    keep_x.start()
    keep_y.start()

    passed = []
    for k in range(1, nd):
        x_out[k - 1].wait_recv()
        source = lax.rem(d + nd - k, nd)
        for j in range(1, nm):
            copy = remote(
                xland.at[source, part],
                xland.at[source, part],
                ms.at[k - 1, j - 1],
                mr.at[k - 1, j - 1],
                {"mp": lax.rem(m + j, nm)},
            )
            copy.start()
            passed.append(copy)
    for k in range(1, nz):
        z_out[k - 1].wait_recv()
        source = 2 * lax.rem(z + nz - k, nz) + x
        copy = remote(yland.at[source], yland.at[source], fs.at[k], fr.at[k], {"dp": other})
        copy.start()
        over.append(copy)
    keep_x.wait()
    keep_y.wait()
    for copy in passed:
        copy.wait_recv()
    for s in range(nd):
        xt[:, s * rows : (s + 1) * rows] = xland[s].T.astype(jnp.bfloat16)
    for copy in over:
        copy.wait_recv()
    for s in range(nd):
        yb[s * rows : (s + 1) * rows, :] = yland[s].astype(jnp.bfloat16)
    width = yb.shape[1]
    tile = 256 if width % 256 == 0 else width

    def body(t, carry):
        cols = pl.ds(pl.multiple_of(t * tile, 128), tile)
        g_ref[:, cols] = scale * jnp.dot(xt[...], yb[:, cols], preferred_element_type=jnp.float32)
        return carry

    lax.fori_loop(0, width // tile, body, 0)
    for copy in x_out + z_out + passed + over:
        copy.wait_send()


def gradient_block(tokens, cotangent, norm_scale):
    nd, nm = lax.axis_size("dp"), lax.axis_size("mp")
    rows, depth = tokens.shape
    width = cotangent.shape[1]
    block = depth // nd
    need = 4 * rows * (depth + width) + 6 * nd * rows * (block + width) + 4 * block * width
    if need > VMEM_BUDGET or nd % 2 or rows % (8 * nm) or block % 128 or width % 128:
        partial = lax.dot_general(
            tokens, cotangent, (((0,), (0,)), ((), ())), preferred_element_type=jnp.float32
        )
        return lax.psum_scatter(partial * norm_scale, "dp", scatter_dimension=0, tiled=True)
    nz = nd // 2
    dma = pltpu.SemaphoreType.DMA
    return pl.pallas_call(
        functools.partial(gradient_kernel, nd, nm, norm_scale),
        out_shape=jax.ShapeDtypeStruct((block, width), jnp.float32),
        in_specs=[pl.BlockSpec(memory_space=VMEM)] * 2,
        out_specs=pl.BlockSpec(memory_space=VMEM),
        scratch_shapes=[
            pltpu.VMEM((nd, rows, block), jnp.float32),
            pltpu.VMEM((nd, rows, width), jnp.float32),
            pltpu.VMEM((block, nd * rows), jnp.bfloat16),
            pltpu.VMEM((nd * rows, width), jnp.bfloat16),
            dma((2,)),
            dma((nd - 1,)),
            dma((nd - 1,)),
            dma((nd - 1, nm - 1)),
            dma((nd - 1, nm - 1)),
            dma((nz - 1,)),
            dma((nz - 1,)),
            dma((nz,)),
            dma((nz,)),
        ],
        compiler_params=pltpu.CompilerParams(
            collective_id=0, has_side_effects=True, vmem_limit_bytes=60 * 2**20
        ),
        name="gradient_block",
    )(tokens.astype(jnp.float32), cotangent.astype(jnp.float32))


def inverse_factor(matrix, identity):
    return lax.linalg.triangular_solve(
        jnp.linalg.cholesky(matrix), identity, left_side=True, lower=True
    )


def shards(tokens, cotangent, sketch):
    rank_size = sketch.shape[1]
    norm_scale = 1.0 / math.sqrt(tokens.shape[0] * lax.axis_size("dp"))
    gradient = gradient_block(tokens, cotangent, norm_scale)
    identity = jnp.eye(rank_size, dtype=jnp.float32)

    def covariance(sketch_proj, grad_proj, ident):
        (summed,) = all_sum((product(gradient, grad_proj),), "mp", ident)
        return DECAY_RATE * product(sketch, sketch_proj) + summed

    grad_proj, sketch_proj = all_sum(
        (product(gradient, sketch, TN), product(sketch, sketch, TN)), "dp", 1
    )
    previous = covariance(sketch_proj, grad_proj, 2)
    grad_image, sketch_image, gram_mat = all_sum(
        (
            product(gradient, previous, TN),
            product(sketch, previous, TN),
            product(previous, previous, TN),
        ),
        "dp",
        3,
    )
    low_inv = inverse_factor(gram_mat, identity)
    applied = covariance(product(sketch_image, low_inv, NT), product(grad_image, low_inv, NT), 4)
    image_grad, cross_prev, self_image = all_sum(
        (
            product(gradient, applied, TN),
            product(previous, applied, TN),
            product(applied, applied, TN),
        ),
        "dp",
        5,
    )
    rayleigh = product(low_inv, cross_prev)
    rayleigh = 0.5 * (rayleigh + rayleigh.T)
    mean_level = jnp.trace(rayleigh) / rank_size
    new_inv = inverse_factor(rayleigh + RIDGE_FRAC * mean_level * identity, identity)
    new_sketch = product(applied, new_inv, NT)
    self_gram = product(product(new_inv, self_image), new_inv, NT)
    inner_inv = inverse_factor(mean_level * identity + self_gram, identity)
    mixer = product(inner_inv, product(inner_inv, new_inv), TN)
    precond = gradient - product(product(new_sketch, mixer), image_grad, NT)
    return (precond.astype(jnp.bfloat16), new_sketch)


def solution(mesh):
    in_specs = (P("dp", None), P("dp", "mp"), P("dp", None))
    out_specs = (P("dp", "mp"), P("dp", None))
    return jax.shard_map(shards, mesh=mesh, in_specs=in_specs, out_specs=out_specs, check_vma=False)
```

```python
import functools
import math

import jax
import jax.numpy as jnp
from jax import lax
from jax.experimental import pallas as pl
from jax.experimental.pallas import tpu as pltpu
from jax.sharding import PartitionSpec as P

DECAY_RATE = 0.9
RIDGE_FRAC = 0.0001
MESH = pl.DeviceIdType.MESH
VMEM = pltpu.MemorySpace.VMEM
VMEM_BUDGET = 48 * 2**20


def product(left_mat, right_mat, dims=((1,), (0,))):
    return lax.dot_general(
        left_mat,
        right_mat,
        (dims, ((), ())),
        precision=lax.Precision.HIGHEST,
        preferred_element_type=jnp.float32,
    )


TN = ((0,), (0,))
NT = ((1,), (1,))


def remote(src, dst, send, recv, where):
    return pltpu.make_async_remote_copy(
        src_ref=src,
        dst_ref=dst,
        send_sem=send,
        recv_sem=recv,
        device_id=where,
        device_id_type=MESH,
    )


def inverse_factor(matrix):
    n = matrix.shape[0]
    start = jnp.where(
        lax.broadcasted_iota(jnp.int32, (n, n), 0) == lax.broadcasted_iota(jnp.int32, (n, n), 1), 1.0, 0.0
    ).astype(jnp.float32)
    left = [matrix[8 * i : 8 * i + 8] for i in range(n // 8)]
    right = [start[8 * i : 8 * i + 8] for i in range(n // 8)]
    row_of = lax.broadcasted_iota(jnp.int32, (8, 1), 0)
    rows = []
    for j in range(0, n, 2):
        t, s = divmod(j, 8)
        a0, a1 = left[t][s : s + 1], left[t][s + 1 : s + 2]
        b0, b1 = right[t][s : s + 1], right[t][s + 1 : s + 2]
        pivot, side, corner = a0[:, j : j + 1], a0[:, j + 1 : j + 2], a1[:, j + 1 : j + 2]
        inv0 = 1.0 / pivot
        factor = side * inv0
        a1, b1 = a1 - factor * a0, b1 - factor * b0
        second = corner - factor * side
        inv1 = 1.0 / second
        rows += [b0 * lax.rsqrt(pivot), b1 * lax.rsqrt(second)]
        a0, b0, a1, b1 = a0 * inv0, b0 * inv0, a1 * inv1, b1 * inv1
        for i in range(t, n // 8):
            c0, c1 = left[i][:, j : j + 1], left[i][:, j + 1 : j + 2]
            c1 = c1 - factor * c0
            if i == t:
                c0 = jnp.where(row_of > s + 1, c0, 0.0)
                c1 = jnp.where(row_of > s + 1, c1, 0.0)
            left[i] = left[i] - c0 * a0 - c1 * a1
            right[i] = right[i] - c0 * b0 - c1 * b1
    return jnp.concatenate(rows, axis=0)


def factor_kernel(matrix_ref, inverse_ref):
    inverse_ref[...] = inverse_factor(matrix_ref[...])


def finish_kernel(low_ref, cross_ref, self_ref, new_ref, mixer_ref):
    rank_size = low_ref.shape[0]
    half = product(low_ref[...], cross_ref[...])
    rayleigh = 0.5 * (half + half.T)
    square = (rank_size, rank_size)
    diagonal = lax.broadcasted_iota(jnp.int32, square, 0) == lax.broadcasted_iota(jnp.int32, square, 1)
    mean_level = jnp.sum(jnp.where(diagonal, rayleigh, 0.0)) / rank_size
    shifted = rayleigh + jnp.where(diagonal, RIDGE_FRAC * mean_level, 0.0)
    new_inv = inverse_factor(shifted)
    new_ref[...] = new_inv
    self_gram = product(product(new_inv, self_ref[...]), new_inv, NT)
    inner_inv = inverse_factor(self_gram + jnp.where(diagonal, mean_level, 0.0))
    mixer_ref[...] = product(inner_inv.T, product(inner_inv, new_inv))


def small_call(kernel, count, name, *arrays):
    shape = jax.ShapeDtypeStruct(arrays[0].shape, jnp.float32)
    return pl.pallas_call(
        kernel,
        out_shape=(shape,) * count,
        in_specs=[pl.BlockSpec(memory_space=VMEM)] * len(arrays),
        out_specs=(pl.BlockSpec(memory_space=VMEM),) * count,
        name=name,
    )(*arrays)


def reduce_kernel(axis, n, with_factor, *refs):
    if with_factor:
        x_ref, matrix_ref, o_ref, inverse_ref, *refs = refs
    else:
        x_ref, o_ref, *refs = refs
    land, own, send_a, recv_a, send_b, recv_b = refs
    me = lax.axis_index(axis)
    chunk = own.shape[0]
    barrier = pltpu.get_barrier_semaphore()
    peers = [lax.rem(me + k, n) for k in range(1, n)]
    for peer in peers:
        pl.semaphore_signal(barrier, inc=1, device_id={axis: peer}, device_id_type=MESH)
    pl.semaphore_wait(barrier, n - 1)
    scatter = [
        remote(
            x_ref.at[pl.ds(pl.multiple_of(peer * chunk, 8), chunk)],
            land.at[k],
            send_a.at[k],
            recv_a.at[k],
            {axis: peer},
        )
        for k, peer in enumerate(peers)
    ]
    for copy in scatter:
        copy.start()
    if with_factor:
        inverse_ref[...] = inverse_factor(matrix_ref[...])
    mine = pl.ds(pl.multiple_of(me * chunk, 8), chunk)
    total = x_ref[mine]
    for k, copy in enumerate(scatter):
        copy.wait_recv()
        total = total + land[k]
    own[...] = total
    gather = [
        remote(own, o_ref.at[mine], send_b.at[k], recv_b.at[k], {axis: peer})
        for k, peer in enumerate(peers)
    ]
    for copy in gather:
        copy.start()
    o_ref[mine] = total
    for copy in scatter:
        copy.wait_send()
    for copy in gather:
        copy.wait()


def all_sum(arrays, axis, ident, matrix=None):
    n = lax.axis_size(axis)
    rows = sum(a.shape[0] for a in arrays)
    if rows % (8 * n) or n > 16:
        summed = lax.psum(tuple(arrays), axis)
        return summed if matrix is None else summed + small_call(factor_kernel, 1, "factor", matrix)
    joined = arrays[0] if len(arrays) == 1 else jnp.concatenate(arrays, axis=0)
    width = joined.shape[1]
    chunk = rows // n
    operands = (joined,) if matrix is None else (joined, matrix)
    summed, *inverse = pl.pallas_call(
        functools.partial(reduce_kernel, axis, n, matrix is not None),
        out_shape=tuple(jax.ShapeDtypeStruct(a.shape, jnp.float32) for a in operands),
        in_specs=[pl.BlockSpec(memory_space=VMEM)] * len(operands),
        out_specs=(pl.BlockSpec(memory_space=VMEM),) * len(operands),
        scratch_shapes=[
            pltpu.VMEM((n - 1, chunk, width), jnp.float32),
            pltpu.VMEM((chunk, width), jnp.float32),
        ]
        + [pltpu.SemaphoreType.DMA((n - 1,))] * 4,
        compiler_params=pltpu.CompilerParams(collective_id=ident, has_side_effects=True),
        name=f"sum_{axis}_{ident}",
    )(*operands)
    outs, at = [], 0
    for a in arrays:
        outs.append(summed[at : at + a.shape[0]])
        at += a.shape[0]
    return tuple(outs + inverse)


def gradient_kernel(
    nd, nm, pieces, scale, x_ref, y_ref, g_ref, xland, yland, xt, yb,
    local, xs, xr, ms, mr, zs, zr, fs, fr, os, orr,
):
    d, m = lax.axis_index("dp"), lax.axis_index("mp")
    rows, block = xland.shape[1], xland.shape[2]
    share = rows // nm
    nz = nd // 2
    z, x = lax.div(d, 2), lax.rem(d, 2)
    other = 2 * z + 1 - x
    barrier = pltpu.get_barrier_semaphore()
    for k in range(1, nd):
        pl.semaphore_signal(barrier, inc=1, device_id={"dp": lax.rem(d + k, nd)}, device_id_type=MESH)
    for k in range(1, nm):
        pl.semaphore_signal(barrier, inc=1, device_id={"mp": lax.rem(m + k, nm)}, device_id_type=MESH)
    pl.semaphore_wait(barrier, nd + nm - 2)

    part = pl.ds(pl.multiple_of(m * share, 8), share)
    x_out = []
    for k in range(1, nd):
        peer = lax.rem(d + k, nd)
        cols = pl.ds(pl.multiple_of(peer * block, 128), block)
        x_out.append(
            remote(x_ref.at[part, cols], xland.at[d, part], xs.at[k - 1], xr.at[k - 1], {"dp": peer})
        )
    piece = rows // pieces
    cuts = [pl.ds(c * piece, piece) for c in range(pieces)]

    def along(way, k, c):
        source = 2 * (z - way * k) + x
        at = yland.at[source, cuts[c]]
        return remote(
            y_ref.at[cuts[c]] if k == 0 else at,
            at,
            zs.at[(way + 1) // 2, k, c],
            zr.at[(way + 1) // 2, k, c],
            {"dp": 2 * (z + way) + x},
        )

    def across(way, k, c):
        at = yland.at[2 * (z - way * (k + 1)) + x, cuts[c]]
        return remote(at, at, fs.at[(way + 1) // 2, k, c], fr.at[(way + 1) // 2, k, c], {"dp": other})

    def inside(place):
        return jnp.logical_and(place >= 0, place < nz)

    def sends(way, k):
        return jnp.logical_and(inside(z - way * k), inside(z + way))

    def streams(steps):
        return [(way, k, c) for k in range(steps) for c in range(pieces) for way in (1, -1)]

    over = [
        remote(y_ref.at[cut], yland.at[d, cut], os.at[c], orr.at[c], {"dp": other})
        for c, cut in enumerate(cuts)
    ]
    for c in range(pieces):
        for way in (1, -1):
            pl.when(sends(way, 0))(lambda way=way, c=c: along(way, 0, c).start())
        over[c].start()
        if c == 0:
            for copy in x_out:
                copy.start()
    mine = pl.ds(pl.multiple_of(d * block, 128), block)
    keep_x = pltpu.make_async_copy(x_ref.at[:, mine], xland.at[d], local.at[0])
    keep_y = pltpu.make_async_copy(y_ref, yland.at[d], local.at[1])
    keep_x.start()
    keep_y.start()

    passed = []
    for k in range(1, nd):
        x_out[k - 1].wait_recv()
        source = lax.rem(d + nd - k, nd)
        for j in range(1, nm):
            copy = remote(
                xland.at[source, part],
                xland.at[source, part],
                ms.at[k - 1, j - 1],
                mr.at[k - 1, j - 1],
                {"mp": lax.rem(m + j, nm)},
            )
            copy.start()
            passed.append(copy)
    for way, k, c in streams(nz - 1):

        @pl.when(inside(z - way * (k + 1)))
        def _():
            along(way, k, c).wait_recv()
            across(way, k, c).start()

            if k + 1 < nz - 1:

                @pl.when(inside(z + way))
                def _():
                    along(way, k + 1, c).start()

    keep_x.wait()
    keep_y.wait()
    for copy in passed:
        copy.wait_recv()
    for s in range(nd):
        xt[:, s * rows : (s + 1) * rows] = xland[s].T.astype(jnp.bfloat16)
    for copy in over:
        copy.wait_recv()
    for way, k, c in streams(nz - 1):
        pl.when(inside(z - way * (k + 1)))(lambda way=way, k=k, c=c: across(way, k, c).wait())
    for s in range(nd):
        yb[s * rows : (s + 1) * rows, :] = yland[s].astype(jnp.bfloat16)
    width = yb.shape[1]
    tile = 256 if width % 256 == 0 else width

    def body(t, carry):
        cols = pl.ds(pl.multiple_of(t * tile, 128), tile)
        g_ref[:, cols] = scale * jnp.dot(xt[...], yb[:, cols], preferred_element_type=jnp.float32)
        return carry

    lax.fori_loop(0, width // tile, body, 0)
    for copy in x_out + passed + over:
        copy.wait_send()
    for way, k, c in streams(nz - 1):
        pl.when(sends(way, k))(lambda way=way, k=k, c=c: along(way, k, c).wait_send())


def gradient_block(tokens, cotangent, norm_scale):
    nd, nm = lax.axis_size("dp"), lax.axis_size("mp")
    rows, depth = tokens.shape
    width = cotangent.shape[1]
    block = depth // nd
    need = 4 * rows * (depth + width) + 6 * nd * rows * (block + width) + 4 * block * width
    if need > VMEM_BUDGET or nd % 2 or rows % (8 * nm) or block % 128 or width % 128:
        partial = lax.dot_general(
            tokens, cotangent, (((0,), (0,)), ((), ())), preferred_element_type=jnp.float32
        )
        return lax.psum_scatter(partial * norm_scale, "dp", scatter_dimension=0, tiled=True)
    nz = nd // 2
    pieces = 2 if rows % 16 == 0 else 1
    dma = pltpu.SemaphoreType.DMA
    return pl.pallas_call(
        functools.partial(gradient_kernel, nd, nm, pieces, norm_scale),
        out_shape=jax.ShapeDtypeStruct((block, width), jnp.float32),
        in_specs=[pl.BlockSpec(memory_space=VMEM)] * 2,
        out_specs=pl.BlockSpec(memory_space=VMEM),
        scratch_shapes=[
            pltpu.VMEM((nd, rows, block), jnp.float32),
            pltpu.VMEM((nd, rows, width), jnp.float32),
            pltpu.VMEM((block, nd * rows), jnp.bfloat16),
            pltpu.VMEM((nd * rows, width), jnp.bfloat16),
            dma((2,)),
            dma((nd - 1,)),
            dma((nd - 1,)),
            dma((nd - 1, nm - 1)),
            dma((nd - 1, nm - 1)),
            dma((2, nz - 1, pieces)),
            dma((2, nz - 1, pieces)),
            dma((2, nz - 1, pieces)),
            dma((2, nz - 1, pieces)),
            dma((pieces,)),
            dma((pieces,)),
        ],
        compiler_params=pltpu.CompilerParams(
            collective_id=0, has_side_effects=True, vmem_limit_bytes=60 * 2**20
        ),
        name="gradient_block",
    )(tokens.astype(jnp.float32), cotangent.astype(jnp.float32))


def shards(tokens, cotangent, sketch):
    norm_scale = 1.0 / math.sqrt(tokens.shape[0] * lax.axis_size("dp"))
    gradient = gradient_block(tokens, cotangent, norm_scale)

    grad_proj, sketch_proj = all_sum(
        (product(gradient, sketch, TN), product(sketch, sketch, TN)), "dp", 1
    )
    (summed,) = all_sum((product(gradient, grad_proj),), "mp", 2)
    previous = DECAY_RATE * product(sketch, sketch_proj) + summed
    grad_image, sketch_image, gram_mat = all_sum(
        (
            product(gradient, previous, TN),
            product(sketch, previous, TN),
            product(previous, previous, TN),
        ),
        "dp",
        3,
    )
    summed, low_inv = all_sum((product(gradient, grad_image),), "mp", 4, gram_mat)
    applied = product(DECAY_RATE * product(sketch, sketch_image) + summed, low_inv, NT)
    image_grad, cross_prev, self_image = all_sum(
        (
            product(gradient, applied, TN),
            product(previous, applied, TN),
            product(applied, applied, TN),
        ),
        "dp",
        5,
    )
    new_inv, mixer = small_call(finish_kernel, 2, "finish", low_inv, cross_prev, self_image)
    new_sketch = product(applied, new_inv, NT)
    precond = gradient - product(product(new_sketch, mixer), image_grad, NT)
    return (precond.astype(jnp.bfloat16), new_sketch)


def solution(mesh):
    in_specs = (P("dp", None), P("dp", "mp"), P("dp", None))
    out_specs = (P("dp", "mp"), P("dp", None))
    return jax.shard_map(shards, mesh=mesh, in_specs=in_specs, out_specs=out_specs, check_vma=False)
```
